32 devices in a mesh: com: 8 (over y, x, core), arc: 4 (over z).
Axes of the slice: x: 2, y: 2, z: 4, core: 2. Of those that a mesh axis runs over, the one named last changes fastest.
Arguments:
- flow_start: float32 [256, 65536], P('com', 'arc'), may hold values from 0 to 1
- price_start: float32 [256, 16384], P('com'), may hold values from -3 to 3
- cost: float32 [256, 65536], P('com', 'arc'), may hold values from -6 to 6
- demand: float32 [256, 16384], P('com'), may hold values from -6 to 6
- head_block: int32 [512], P('arc'), may hold values from 0 to 127
- tail_block: int32 [512], P('arc'), may hold values from 0 to 127
- head_local: int32 [65536], P('arc'), may hold values from 0 to 127
- tail_local: int32 [65536], P('arc'), may hold values from 0 to 127
- cap_class: int32 [65536], P('arc'), may hold values from 0 to 7
- cap_levels: float32 [8], replicated, may hold values from 25 to 128
Outputs:
- flow: float32 [256, 65536], P('com', 'arc')
- price: float32 [256, 16384], P('com')
The draws below stay inside these ranges and needn't reach their ends.
Inputs may be any that keep to these rules, and one draw needn't show every extreme that they name: `head_block`: node block indices. `tail_block`: node block indices. `head_local`: positions within a node block. `tail_local`: positions within a node block.
All inputs are finite; a program needn't handle non-finite values.
Results may differ from the reference program's by a relative error of at most 0.00016.
Values sent between devices are 32-bit elements; how exact they have to be, the bound alone decides.
A program may use at most 128 MiB of HBM per device.

```python
import math
import jax
import jax.numpy as jnp

NODES = 16384
BLOCK = 128
CLASSES = 8
ITERS = 4
NEWTON = 3
COMMODITIES = 256
ARCS = 65536
ARC_BLOCKS = 512
NODE_BLOCKS = 128


def set_ends(result, key, low, largest):
    longest = result.shape.index(max(result.shape))
    spots = []
    for shift in (0, 1):
        where = [jax.random.randint(jax.random.fold_in(key, axis), (), 0, length) for axis, length in enumerate(result.shape)]
        where[longest] = (where[longest] + shift) % result.shape[longest]
        spots.append(tuple(where))
    return result.at[spots[0]].set(low).at[spots[1]].set(largest)


def shard_levels(key, extent, shards, low, largest):
    def one(dim, blocks):
        heights = jax.random.uniform(jax.random.fold_in(jax.random.fold_in(key, 6), dim), (blocks,), jnp.float32, low / len(shards), largest / len(shards))
        return jnp.repeat(jnp.exp(heights), extent[dim] // blocks).reshape((-1,) + (1,) * (len(extent) - dim - 1))

    factor_of = one(*shards[0])
    for cut in shards[1:]:
        factor_of = factor_of * one(*cut)
    return factor_of


def noise(own_key, shape, width, reach, cuts=(), held_as=jnp.bfloat16):
    result = jax.random.normal(own_key, shape, jnp.float32) * width
    if len(cuts) > 0:
        result = shard_levels(own_key, shape, cuts, -0.22, 0.18) * result
    return jnp.clip(result, min=-reach, max=reach).astype(held_as)


def setup_inputs(seed: int = 0) -> dict:
    keys = jax.random.split(jax.random.key(seed), 11)
    return {
        "flow_start": jnp.clip(1.0 * jax.random.uniform(keys[0], (COMMODITIES, ARCS), jnp.float32) ** shard_levels(keys[0], (COMMODITIES, ARCS), ((0, 8), (1, 4)), -0.2, 0.2), 0.0, 1.0),
        "price_start": noise(keys[1], (COMMODITIES, NODES), 0.5, 3.0, ((0, 8),), jnp.float32),
        "cost": noise(keys[2], (COMMODITIES, ARCS), 1.0, 6.0, ((0, 8), (1, 4)), jnp.float32),
        "demand": noise(keys[3], (COMMODITIES, NODES), 1.0, 6.0, ((0, 8),), jnp.float32),
        "head_block": set_ends(jax.random.randint(keys[4], (ARC_BLOCKS,), 0, NODE_BLOCKS), jax.random.fold_in(keys[4], 1), 0, NODE_BLOCKS - 1).astype(jnp.int32),
        "tail_block": set_ends(jax.random.randint(keys[5], (ARC_BLOCKS,), 0, NODE_BLOCKS), jax.random.fold_in(keys[5], 1), 0, NODE_BLOCKS - 1).astype(jnp.int32),
        "head_local": set_ends(jax.random.randint(keys[6], (ARCS,), 0, BLOCK), jax.random.fold_in(keys[6], 1), 0, BLOCK - 1).astype(jnp.int32),
        "tail_local": set_ends(jax.random.randint(keys[7], (ARCS,), 0, BLOCK), jax.random.fold_in(keys[7], 1), 0, BLOCK - 1).astype(jnp.int32),
        "cap_class": set_ends(jax.random.randint(keys[8], (ARCS,), 0, CLASSES), jax.random.fold_in(keys[8], 1), 0, CLASSES - 1).astype(jnp.int32),
        "cap_levels": jnp.clip(jnp.exp(jax.random.uniform(keys[9], (CLASSES,), jnp.float32, math.log(25.0), math.log(128.0))), 25.0, 128.0),
    }


step_primal = 0.25
step_dual = 0.1
soft_width = 0.05


def reference(flow_start, price_start, cost, demand, head_block, tail_block, head_local, tail_local, cap_class, cap_levels):
    heads = (jnp.repeat(head_block, BLOCK) * BLOCK + head_local).astype(jnp.int32)
    tails = (jnp.repeat(tail_block, BLOCK) * BLOCK + tail_local).astype(jnp.int32)
    capacity = cap_levels[cap_class]
    flow = flow_start
    price = price_start
    for step in range(ITERS):
        trial = flow - step_primal * (cost - (price[:, heads] - price[:, tails]))
        theta = jnp.zeros((trial.shape[1],), jnp.float32)
        for inner in range(NEWTON):
            excess = jnp.maximum(trial - theta, 0.0)
            total = jnp.sum(excess, axis=0)
            active = jnp.sum(jnp.minimum(excess / soft_width, 1.0), axis=0)
            theta = theta + jnp.maximum(total - capacity, 0.0) / jnp.maximum(active, 1.0)
        fresh = jnp.maximum(trial - theta, 0.0)
        extra = (2.0 * fresh - flow).T
        balance = jax.ops.segment_sum(extra, heads, NODES) - jax.ops.segment_sum(extra, tails, NODES)
        price = price + step_dual * (demand - balance.T)
        flow = fresh
    return flow, price
```

```python
import functools

import jax
import jax.numpy as jnp
from jax import lax
from jax.experimental import pallas as pl
from jax.experimental.pallas import tpu as pltpu
from jax.sharding import PartitionSpec as P

BLOCK = 128
CLASSES = 8
ITERS = 4
NEWTON = 3
CHUNKS = 32
LAG = 2
MIB = 1 << 20

step_primal = 0.25
step_dual = 0.1
soft_width = 0.05
VMEM = pltpu.VMEM
SMEM = pltpu.SMEM
MESH = pl.DeviceIdType.MESH


def two_parts(x):
    high = x.astype(jnp.bfloat16)
    low = (x - high.astype(jnp.float32)).astype(jnp.bfloat16)
    return jnp.concatenate([high, low], axis=0)


def one_hot_rows(local_row):
    nodes = lax.broadcasted_iota(jnp.int32, (BLOCK, BLOCK), 0)
    return jnp.where(nodes == local_row, 1.0, 0.0).astype(jnp.bfloat16)


def lanes_of(block):
    return pl.ds(pl.multiple_of(block * BLOCK, BLOCK), BLOCK)


def put_sums(sums, where, within, excess):
    sums[*where, 0, pl.ds(within, 1), :] = jnp.sum(excess, axis=0, keepdims=True)
    sums[*where, 1, pl.ds(within, 1), :] = jnp.sum(
        jnp.minimum(excess * (1.0 / soft_width), 1.0), axis=0, keepdims=True
    )


def trial_kernel(
    head_block, tail_block, flow, price, cost, head_local, tail_local, trial, sums
):
    rows = flow.shape[0]
    group, _, per, _ = sums.shape
    unroll = min(per, 8)

    def some(k, carry):
        for u in range(unroll):
            block = k * unroll + u
            at_head = price[:, lanes_of(head_block[block])]
            at_tail = price[:, lanes_of(tail_block[block])]
            left = jnp.concatenate([two_parts(at_head), two_parts(at_tail)], axis=1)
            right = jnp.concatenate(
                [
                    one_hot_rows(head_local[pl.ds(block, 1), :]),
                    -one_hot_rows(tail_local[pl.ds(block, 1), :]),
                ],
                axis=0,
            )
            both = jnp.dot(left, right, preferred_element_type=jnp.float32)
            here = lanes_of(block)
            value = flow[:, here] - step_primal * (cost[:, here] - (both[:rows] + both[rows:]))
            trial[:, here] = value
            put_sums(sums, (block // per,), block % per, jnp.maximum(value, 0.0))
        return carry

    lax.fori_loop(0, group * per // unroll, some, 0)


def project_kernel(
    group,
    levels,
    trial,
    first_sums,
    cap_class,
    fresh,
    sums,
    partial,
    theta,
    sum_send,
    sum_recv,
    theta_send,
    theta_recv,
):
    me = lax.axis_index("com")
    blocks = trial.shape[1] // BLOCK
    per = blocks // group

    barrier = pltpu.get_barrier_semaphore()
    for s in range(1, group):
        pl.semaphore_signal(
            barrier, inc=1, device_id={"com": lax.rem(me + s, group)}, device_id_type=MESH
        )
    pl.semaphore_wait(barrier, group - 1)

    def own_sums(step, owner):
        return sums.at[step - 1, owner] if step else first_sums.at[owner]

    def sum_copy(step, s):
        peer = lax.rem(me + group - s, group)
        return pltpu.make_async_remote_copy(
            src_ref=own_sums(step, peer),
            dst_ref=partial.at[step, s],
            send_sem=sum_send.at[step, s],
            recv_sem=sum_recv.at[step, s],
            device_id={"com": peer},
            device_id_type=MESH,
        )

    def theta_copy(step, s):
        return pltpu.make_async_remote_copy(
            src_ref=theta.at[step, me],
            dst_ref=theta.at[step, me],
            send_sem=theta_send.at[step, s],
            recv_sem=theta_recv.at[step, s],
            device_id={"com": lax.rem(me + s, group)},
            device_id_type=MESH,
        )

    unroll = min(per, 8)

    def each_block(owner, body):
        def some(k, carry):
            for u in range(unroll):
                within = k * unroll + u
                body(owner * per + within, within)
            return carry

        lax.fori_loop(0, per // unroll, some, 0)

    for s in range(1, group):
        sum_copy(0, s).start()

    kinds = cap_class[me]
    capacity = jnp.zeros(kinds.shape, jnp.float32)
    for c in range(CLASSES):
        capacity = capacity + jnp.where(kinds == c, levels[c], 0.0)

    for step in range(NEWTON):
        both = own_sums(step, me)[...]
        for s in range(1, group):
            sum_copy(step, s).wait_recv()
            both = both + partial[step, s]
        mine = jnp.maximum(both[0] - capacity, 0.0) / jnp.maximum(both[1], 1.0)
        if step:
            mine = theta[step - 1, me] + mine
        theta[step, me] = mine
        for s in range(1, group):
            theta_copy(step, s).start()
        for s in range(group):
            owner = lax.rem(me + group - s, group)
            if s:
                theta_copy(step, s).wait_recv()

            def later(block, within, owner=owner, step=step):
                here = lanes_of(block)
                excess = jnp.maximum(
                    trial[:, here] - theta[step, owner, pl.ds(within, 1), :], 0.0
                )
                if step < NEWTON - 1:
                    put_sums(sums, (step, owner), within, excess)
                else:
                    fresh[:, here] = excess

            each_block(owner, later)
            if s and step < NEWTON - 1:
                sum_copy(step + 1, s).start()
    for step in range(NEWTON):
        for s in range(1, group):
            sum_copy(step, s).wait_send()
            theta_copy(step, s).wait_send()


def spread_kernel(head_block, tail_block, flow, fresh, head_local, tail_local, balance):
    rows = flow.shape[0]
    blocks = flow.shape[1] // BLOCK
    unroll = 8
    balance[...] = jnp.zeros_like(balance)

    def some(k, carry):
        results = []
        for u in range(unroll):
            block = k * unroll + u
            here = lanes_of(block)
            left = two_parts(2.0 * fresh[:, here] - flow[:, here])
            right = jnp.concatenate(
                [
                    one_hot_rows(head_local[pl.ds(block, 1), :]),
                    -one_hot_rows(tail_local[pl.ds(block, 1), :]),
                ],
                axis=0,
            )
            both = lax.dot_general(
                left, right, (((1,), (1,)), ((), ())), preferred_element_type=jnp.float32
            )
            results.append(both[:rows] + both[rows:])
        for u in range(unroll):
            block = k * unroll + u
            head, tail = lanes_of(head_block[block]), lanes_of(tail_block[block])
            balance[:, head] += results[u][:, :BLOCK]
            balance[:, tail] += results[u][:, BLOCK:]
        return carry

    lax.fori_loop(0, blocks // unroll, some, 0)


def price_kernel(
    line,
    balance,
    price,
    demand,
    out,
    from_left,
    from_right,
    to_right,
    to_left,
    right_send,
    right_recv,
    left_send,
    left_recv,
):
    me = lax.axis_index("arc")
    width = balance.shape[1] // CHUNKS
    first, last = me == 0, me == line - 1
    inner = jnp.logical_and(me > 0, me < line - 1)
    right, left = lax.rem(me + 1, line), lax.rem(me + line - 1, line)

    barrier = pltpu.get_barrier_semaphore()

    @pl.when(me > 0)
    def _():
        pl.semaphore_signal(barrier, inc=1, device_id={"arc": left}, device_id_type=MESH)

    @pl.when(me < line - 1)
    def _():
        pl.semaphore_signal(barrier, inc=1, device_id={"arc": right}, device_id_type=MESH)

    @pl.when(inner)
    def _():
        pl.semaphore_wait(barrier, 2)

    @pl.when(jnp.logical_not(inner))
    def _():
        pl.semaphore_wait(barrier, 1)

    def span(c):
        return pl.ds(pl.multiple_of(c * width, BLOCK), width)

    def copy(source, target, send, recv, c, peer):
        return pltpu.make_async_remote_copy(
            src_ref=source.at[:, span(c)],
            dst_ref=target.at[:, span(c)],
            send_sem=send.at[c],
            recv_sem=recv.at[c],
            device_id={"arc": peer},
            device_id_type=MESH,
        )

    def rightward(source, c):
        return copy(source, from_left, right_send, right_recv, c, right)

    def leftward(source, c):
        return copy(source, from_right, left_send, left_recv, c, left)

    def go_right(c):
        @pl.when(first)
        def _():
            rightward(balance, c).start()

        @pl.when(me > 0)
        def _():
            rightward(to_right, c).wait_recv()

        @pl.when(inner)
        def _():
            to_right[:, span(c)] = from_left[:, span(c)] + balance[:, span(c)]
            rightward(to_right, c).start()

    def go_left(c):
        @pl.when(last)
        def _():
            leftward(balance, c).start()

        @pl.when(me < line - 1)
        def _():
            leftward(to_left, c).wait_recv()

        @pl.when(inner)
        def _():
            to_left[:, span(c)] = from_right[:, span(c)] + balance[:, span(c)]
            leftward(to_left, c).start()

    def finish(c):
        def put(total):
            out[:, span(c)] = price[:, span(c)] + step_dual * (demand[:, span(c)] - total)

        @pl.when(first)
        def _():
            put(balance[:, span(c)] + from_right[:, span(c)])

        @pl.when(last)
        def _():
            put(balance[:, span(c)] + from_left[:, span(c)])

        @pl.when(inner)
        def _():
            put(to_right[:, span(c)] + from_right[:, span(c)])

    def sweep(near, far):
        for c in range(LAG):
            near(c)

        def body(c, carry):
            near(c + LAG)
            far(c)
            finish(c)
            return carry

        lax.fori_loop(0, CHUNKS - LAG, body, 0)
        for c in range(CHUNKS - LAG, CHUNKS):
            far(c)
            finish(c)

    @pl.when(me * 2 < line)
    def _():
        sweep(go_right, go_left)

    @pl.when(me * 2 >= line)
    def _():
        sweep(go_left, go_right)

    @pl.when(me < line - 1)
    def _():
        def body(c, carry):
            rightward(to_right, c).wait_send()
            return carry

        lax.fori_loop(0, CHUNKS, body, 0)

    @pl.when(me > 0)
    def _():
        def body(c, carry):
            leftward(to_left, c).wait_send()
            return carry

        lax.fori_loop(0, CHUNKS, body, 0)


def specs(*spaces):
    return [pl.BlockSpec(memory_space=space) for space in spaces]


def on_device(
    group,
    line,
    flow_start,
    price_start,
    cost,
    demand,
    head_block,
    tail_block,
    head_local,
    tail_local,
    cap_class,
    cap_levels,
):
    com_rows, arc_cols = flow_start.shape
    nodes = price_start.shape[1]
    blocks = arc_cols // BLOCK
    per = blocks // group
    heads = head_local.reshape(blocks, BLOCK)
    tails = tail_local.reshape(blocks, BLOCK)
    kinds = cap_class.reshape(group, per, BLOCK)
    dma = pltpu.SemaphoreType.DMA
    wide = jax.ShapeDtypeStruct((com_rows, arc_cols), jnp.float32)
    node = jax.ShapeDtypeStruct((com_rows, nodes), jnp.float32)

    gather = pl.pallas_call(
        trial_kernel,
        out_shape=(wide, jax.ShapeDtypeStruct((group, 2, per, BLOCK), jnp.float32)),
        in_specs=specs(SMEM, SMEM, VMEM, VMEM, VMEM, VMEM, VMEM),
        out_specs=tuple(specs(VMEM, VMEM)),
        compiler_params=pltpu.CompilerParams(vmem_limit_bytes=24 * MIB),
        name="gather",
    )
    project = pl.pallas_call(
        functools.partial(project_kernel, group),
        out_shape=wide,
        in_specs=specs(SMEM, VMEM, VMEM, VMEM),
        out_specs=pl.BlockSpec(memory_space=VMEM),
        scratch_shapes=[
            pltpu.VMEM((NEWTON - 1, group, 2, per, BLOCK), jnp.float32),
            pltpu.VMEM((NEWTON, group, 2, per, BLOCK), jnp.float32),
            pltpu.VMEM((NEWTON, group, per, BLOCK), jnp.float32),
            dma((NEWTON, group)),
            dma((NEWTON, group)),
            dma((NEWTON, group)),
            dma((NEWTON, group)),
        ],
        compiler_params=pltpu.CompilerParams(
            collective_id=0, has_side_effects=True, vmem_limit_bytes=24 * MIB
        ),
        name="project",
    )
    spread = pl.pallas_call(
        spread_kernel,
        out_shape=node,
        in_specs=specs(SMEM, SMEM, VMEM, VMEM, VMEM, VMEM),
        out_specs=pl.BlockSpec(memory_space=VMEM),
        compiler_params=pltpu.CompilerParams(vmem_limit_bytes=24 * MIB),
        name="spread",
    )
    advance = pl.pallas_call(
        functools.partial(price_kernel, line),
        out_shape=node,
        in_specs=specs(VMEM, VMEM, VMEM),
        out_specs=pl.BlockSpec(memory_space=VMEM),
        scratch_shapes=[pltpu.VMEM((com_rows, nodes), jnp.float32)] * 4
        + [dma((CHUNKS,))] * 4,
        compiler_params=pltpu.CompilerParams(
            collective_id=1, has_side_effects=True, vmem_limit_bytes=24 * MIB
        ),
        name="advance",
    )
    flow, price = flow_start, price_start
    for _ in range(ITERS):
        trial, sums = gather(head_block, tail_block, flow, price, cost, heads, tails)
        fresh = project(cap_levels, trial, sums, kinds)
        balance = spread(head_block, tail_block, flow, fresh, heads, tails)
        price = advance(balance, price, demand)
        flow = fresh
    return flow, price


def solution(mesh):
    return jax.shard_map(
        functools.partial(on_device, mesh.shape["com"], mesh.shape["arc"]),
        mesh=mesh,
        in_specs=(
            P("com", "arc"),
            P("com", None),
            P("com", "arc"),
            P("com", None),
            P("arc"),
            P("arc"),
            P("arc"),
            P("arc"),
            P("arc"),
            P(),
        ),
        out_specs=(P("com", "arc"), P("com", None)),
        check_vma=False,
    )
```

```python
import functools

import jax
import jax.numpy as jnp
from jax import lax
from jax.experimental import pallas as pl
from jax.experimental.pallas import tpu as pltpu
from jax.sharding import PartitionSpec as P

BLOCK = 128
CLASSES = 8
ITERS = 4
NEWTON = 3
CHUNKS = 32
EDGE_LAG = 24
INNER_LAG = 2
MIB = 1 << 20

step_primal = 0.25
step_dual = 0.1
soft_width = 0.05
VMEM = pltpu.VMEM
SMEM = pltpu.SMEM
MESH = pl.DeviceIdType.MESH


def two_parts(x):
    high = x.astype(jnp.bfloat16)
    low = (x - high.astype(jnp.float32)).astype(jnp.bfloat16)
    return jnp.concatenate([high, low], axis=0)


def one_hot_rows(local_row):
    nodes = lax.broadcasted_iota(jnp.int32, (BLOCK, BLOCK), 0)
    return jnp.where(nodes == local_row, 1.0, 0.0).astype(jnp.bfloat16)


def lanes_of(block):
    return pl.ds(pl.multiple_of(block * BLOCK, BLOCK), BLOCK)


def put_sums(sums, where, within, excess):
    sums[*where, 0, pl.ds(within, 1), :] = jnp.sum(excess, axis=0, keepdims=True)
    sums[*where, 1, pl.ds(within, 1), :] = jnp.sum(
        jnp.minimum(excess * (1.0 / soft_width), 1.0), axis=0, keepdims=True
    )


def trial_kernel(
    head_block, tail_block, flow, price, cost, head_local, tail_local, trial, sums
):
    rows = flow.shape[0]
    group, _, per, _ = sums.shape
    unroll = min(per, 8)

    def some(k, carry):
        for u in range(unroll):
            block = k * unroll + u
            at_head = price[:, lanes_of(head_block[block])]
            at_tail = price[:, lanes_of(tail_block[block])]
            left = jnp.concatenate([two_parts(at_head), two_parts(at_tail)], axis=1)
            right = jnp.concatenate(
                [
                    one_hot_rows(head_local[pl.ds(block, 1), :]),
                    -one_hot_rows(tail_local[pl.ds(block, 1), :]),
                ],
                axis=0,
            )
            both = jnp.dot(left, right, preferred_element_type=jnp.float32)
            here = lanes_of(block)
            value = flow[:, here] - step_primal * (cost[:, here] - (both[:rows] + both[rows:]))
            trial[:, here] = value
            put_sums(sums, (block // per,), block % per, jnp.maximum(value, 0.0))
        return carry

    lax.fori_loop(0, group * per // unroll, some, 0)


def project_kernel(
    group,
    levels,
    trial,
    first_sums,
    cap_class,
    fresh,
    sums,
    partial,
    theta,
    sum_send,
    sum_recv,
    theta_send,
    theta_recv,
):
    me = lax.axis_index("com")
    blocks = trial.shape[1] // BLOCK
    per = blocks // group

    barrier = pltpu.get_barrier_semaphore()
    for s in range(1, group):
        pl.semaphore_signal(
            barrier, inc=1, device_id={"com": lax.rem(me + s, group)}, device_id_type=MESH
        )
    pl.semaphore_wait(barrier, group - 1)

    def own_sums(step, owner):
        return sums.at[step - 1, owner] if step else first_sums.at[owner]

    def sum_copy(step, s):
        peer = lax.rem(me + group - s, group)
        return pltpu.make_async_remote_copy(
            src_ref=own_sums(step, peer),
            dst_ref=partial.at[step, s],
            send_sem=sum_send.at[step, s],
            recv_sem=sum_recv.at[step, s],
            device_id={"com": peer},
            device_id_type=MESH,
        )

    def theta_copy(step, s):
        return pltpu.make_async_remote_copy(
            src_ref=theta.at[step, me],
            dst_ref=theta.at[step, me],
            send_sem=theta_send.at[step, s],
            recv_sem=theta_recv.at[step, s],
            device_id={"com": lax.rem(me + s, group)},
            device_id_type=MESH,
        )

    unroll = min(per, 8)

    def each_block(owner, body):
        def some(k, carry):
            for u in range(unroll):
                within = k * unroll + u
                body(owner * per + within, within)
            return carry

        lax.fori_loop(0, per // unroll, some, 0)

    for s in range(1, group):
        sum_copy(0, s).start()

    kinds = cap_class[me]
    capacity = jnp.zeros(kinds.shape, jnp.float32)
    for c in range(CLASSES):
        capacity = capacity + jnp.where(kinds == c, levels[c], 0.0)

    for step in range(NEWTON):
        both = own_sums(step, me)[...]
        for s in range(1, group):
            sum_copy(step, s).wait_recv()
            both = both + partial[step, s]
        mine = jnp.maximum(both[0] - capacity, 0.0) / jnp.maximum(both[1], 1.0)
        if step:
            mine = theta[step - 1, me] + mine
        theta[step, me] = mine
        for s in range(1, group):
            theta_copy(step, s).start()
        for s in range(group):
            owner = lax.rem(me + group - s, group)
            if s:
                theta_copy(step, s).wait_recv()

            def later(block, within, owner=owner, step=step):
                here = lanes_of(block)
                excess = jnp.maximum(
                    trial[:, here] - theta[step, owner, pl.ds(within, 1), :], 0.0
                )
                if step < NEWTON - 1:
                    put_sums(sums, (step, owner), within, excess)
                else:
                    fresh[:, here] = excess

            each_block(owner, later)
            if s and step < NEWTON - 1:
                sum_copy(step + 1, s).start()
    for step in range(NEWTON):
        for s in range(1, group):
            sum_copy(step, s).wait_send()
            theta_copy(step, s).wait_send()


def spread_kernel(head_block, tail_block, flow, fresh, head_local, tail_local, balance):
    rows = flow.shape[0]
    blocks = flow.shape[1] // BLOCK
    unroll = 8
    balance[...] = jnp.zeros_like(balance)

    def some(k, carry):
        results = []
        for u in range(unroll):
            block = k * unroll + u
            here = lanes_of(block)
            left = two_parts(2.0 * fresh[:, here] - flow[:, here])
            right = jnp.concatenate(
                [
                    one_hot_rows(head_local[pl.ds(block, 1), :]),
                    -one_hot_rows(tail_local[pl.ds(block, 1), :]),
                ],
                axis=0,
            )
            both = lax.dot_general(
                left, right, (((1,), (1,)), ((), ())), preferred_element_type=jnp.float32
            )
            results.append(both[:rows] + both[rows:])
        for u in range(unroll):
            block = k * unroll + u
            head, tail = lanes_of(head_block[block]), lanes_of(tail_block[block])
            balance[:, head] += results[u][:, :BLOCK]
            balance[:, tail] += results[u][:, BLOCK:]
        return carry

    lax.fori_loop(0, blocks // unroll, some, 0)


def price_kernel(
    line,
    balance,
    price,
    demand,
    out,
    from_left,
    from_right,
    to_right,
    to_left,
    right_send,
    right_recv,
    left_send,
    left_recv,
):
    me = lax.axis_index("arc")
    width = balance.shape[1] // CHUNKS
    first, last = me == 0, me == line - 1
    inner = jnp.logical_and(me > 0, me < line - 1)
    right, left = lax.rem(me + 1, line), lax.rem(me + line - 1, line)

    barrier = pltpu.get_barrier_semaphore()

    @pl.when(me > 0)
    def _():
        pl.semaphore_signal(barrier, inc=1, device_id={"arc": left}, device_id_type=MESH)

    @pl.when(me < line - 1)
    def _():
        pl.semaphore_signal(barrier, inc=1, device_id={"arc": right}, device_id_type=MESH)

    @pl.when(inner)
    def _():
        pl.semaphore_wait(barrier, 2)

    @pl.when(jnp.logical_not(inner))
    def _():
        pl.semaphore_wait(barrier, 1)

    def span(c):
        return pl.ds(pl.multiple_of(c * width, BLOCK), width)

    def copy(source, target, send, recv, c, peer):
        return pltpu.make_async_remote_copy(
            src_ref=source.at[:, span(c)],
            dst_ref=target.at[:, span(c)],
            send_sem=send.at[c],
            recv_sem=recv.at[c],
            device_id={"arc": peer},
            device_id_type=MESH,
        )

    def rightward(source, c):
        return copy(source, from_left, right_send, right_recv, c, right)

    def leftward(source, c):
        return copy(source, from_right, left_send, left_recv, c, left)

    def go_right(c):
        @pl.when(first)
        def _():
            rightward(balance, c).start()

        @pl.when(me > 0)
        def _():
            rightward(to_right, c).wait_recv()

        @pl.when(inner)
        def _():
            to_right[:, span(c)] = from_left[:, span(c)] + balance[:, span(c)]
            rightward(to_right, c).start()

    def go_left(c):
        @pl.when(last)
        def _():
            leftward(balance, c).start()

        @pl.when(me < line - 1)
        def _():
            leftward(to_left, c).wait_recv()

        @pl.when(inner)
        def _():
            to_left[:, span(c)] = from_right[:, span(c)] + balance[:, span(c)]
            leftward(to_left, c).start()

    def finish(c):
        def put(total):
            out[:, span(c)] = price[:, span(c)] + step_dual * (demand[:, span(c)] - total)

        @pl.when(first)
        def _():
            put(balance[:, span(c)] + from_right[:, span(c)])

        @pl.when(last)
        def _():
            put(balance[:, span(c)] + from_left[:, span(c)])

        @pl.when(inner)
        def _():
            put(to_right[:, span(c)] + from_right[:, span(c)])

    def sweep(near, far, lag):
        def ahead(c, carry):
            near(c)
            return carry

        def both(c, carry):
            near(c + lag)
            far(c)
            finish(c)
            return carry

        def behind(c, carry):
            far(c)
            finish(c)
            return carry

        lax.fori_loop(0, lag, ahead, 0)
        lax.fori_loop(0, CHUNKS - lag, both, 0)
        lax.fori_loop(CHUNKS - lag, CHUNKS, behind, 0)

    @pl.when(first)
    def _():
        sweep(go_right, go_left, EDGE_LAG)

    @pl.when(last)
    def _():
        sweep(go_left, go_right, EDGE_LAG)

    @pl.when(jnp.logical_and(inner, me * 2 < line))
    def _():
        sweep(go_right, go_left, INNER_LAG)

    @pl.when(jnp.logical_and(inner, me * 2 >= line))
    def _():
        sweep(go_left, go_right, INNER_LAG)

    @pl.when(me < line - 1)
    def _():
        def body(c, carry):
            rightward(to_right, c).wait_send()
            return carry

        lax.fori_loop(0, CHUNKS, body, 0)

    @pl.when(me > 0)
    def _():
        def body(c, carry):
            leftward(to_left, c).wait_send()
            return carry

        lax.fori_loop(0, CHUNKS, body, 0)


def specs(*spaces):
    return [pl.BlockSpec(memory_space=space) for space in spaces]


def on_device(
    group,
    line,
    flow_start,
    price_start,
    cost,
    demand,
    head_block,
    tail_block,
    head_local,
    tail_local,
    cap_class,
    cap_levels,
):
    com_rows, arc_cols = flow_start.shape
    nodes = price_start.shape[1]
    blocks = arc_cols // BLOCK
    per = blocks // group
    heads = head_local.reshape(blocks, BLOCK)
    tails = tail_local.reshape(blocks, BLOCK)
    kinds = cap_class.reshape(group, per, BLOCK)
    dma = pltpu.SemaphoreType.DMA
    wide = jax.ShapeDtypeStruct((com_rows, arc_cols), jnp.float32)
    node = jax.ShapeDtypeStruct((com_rows, nodes), jnp.float32)

    gather = pl.pallas_call(
        trial_kernel,
        out_shape=(wide, jax.ShapeDtypeStruct((group, 2, per, BLOCK), jnp.float32)),
        in_specs=specs(SMEM, SMEM, VMEM, VMEM, VMEM, VMEM, VMEM),
        out_specs=tuple(specs(VMEM, VMEM)),
        compiler_params=pltpu.CompilerParams(vmem_limit_bytes=24 * MIB),
        name="gather",
    )
    project = pl.pallas_call(
        functools.partial(project_kernel, group),
        out_shape=wide,
        in_specs=specs(SMEM, VMEM, VMEM, VMEM),
        out_specs=pl.BlockSpec(memory_space=VMEM),
        scratch_shapes=[
            pltpu.VMEM((NEWTON - 1, group, 2, per, BLOCK), jnp.float32),
            pltpu.VMEM((NEWTON, group, 2, per, BLOCK), jnp.float32),
            pltpu.VMEM((NEWTON, group, per, BLOCK), jnp.float32),
            dma((NEWTON, group)),
            dma((NEWTON, group)),
            dma((NEWTON, group)),
            dma((NEWTON, group)),
        ],
        compiler_params=pltpu.CompilerParams(
            collective_id=0, has_side_effects=True, vmem_limit_bytes=24 * MIB
        ),
        name="project",
    )
    spread = pl.pallas_call(
        spread_kernel,
        out_shape=node,
        in_specs=specs(SMEM, SMEM, VMEM, VMEM, VMEM, VMEM),
        out_specs=pl.BlockSpec(memory_space=VMEM),
        compiler_params=pltpu.CompilerParams(vmem_limit_bytes=24 * MIB),
        name="spread",
    )
    advance = pl.pallas_call(
        functools.partial(price_kernel, line),
        out_shape=node,
        in_specs=specs(VMEM, VMEM, VMEM),
        out_specs=pl.BlockSpec(memory_space=VMEM),
        scratch_shapes=[pltpu.VMEM((com_rows, nodes), jnp.float32)] * 4
        + [dma((CHUNKS,))] * 4,
        compiler_params=pltpu.CompilerParams(
            collective_id=1, has_side_effects=True, vmem_limit_bytes=24 * MIB
        ),
        name="advance",
    )
    flow, price = flow_start, price_start
    for _ in range(ITERS):
        trial, sums = gather(head_block, tail_block, flow, price, cost, heads, tails)
        fresh = project(cap_levels, trial, sums, kinds)
        balance = spread(head_block, tail_block, flow, fresh, heads, tails)
        price = advance(balance, price, demand)
        flow = fresh
    return flow, price


def solution(mesh):
    return jax.shard_map(
        functools.partial(on_device, mesh.shape["com"], mesh.shape["arc"]),
        mesh=mesh,
        in_specs=(
            P("com", "arc"),
            P("com", None),
            P("com", "arc"),
            P("com", None),
            P("arc"),
            P("arc"),
            P("arc"),
            P("arc"),
            P("arc"),
            P(),
        ),
        out_specs=(P("com", "arc"), P("com", None)),
        check_vma=False,
    )
```
